32 devices in a mesh: band: 8 (over y, x, core), lev: 4 (over z).
Axes of the slice: x: 2, y: 2, z: 4, core: 2. Of those that a mesh axis runs over, the one named last changes fastest.
Arguments:
- spectral: float32 [2, 32, 640, 640], P(None, None, 'band', 'lev'), may hold values from -0.2 to 0.2
- legendre: bfloat16 [640, 640, 640], P('band', 'lev'), may hold values from -0.25 to 0.25
- wave_order: int32 [640], replicated, may hold values from 0 to 639, each once
- jacobian: bfloat16 [32, 640, 1280], P('lev', 'band'), may hold values from 0.5 to 1.5
- obs_cell: int32 [4, 8, 2048], P('lev', 'band'), may hold values from 0 to 819199
- innovation: float32 [4, 8, 2048], P('lev', 'band'), may hold values from -6 to 6
- obs_weight: float32 [4, 8, 2048], P('lev', 'band'), may hold values from 0.01 to 0.04
- inv_var: float32 [640], P('lev'), may hold values from 5 to 50
Outputs:
- model_grid: bfloat16 [32, 640, 1280], P('lev', 'band')
- gradient: float32 [2, 32, 640, 640], P(None, None, 'band', 'lev')
The draws below stay inside these ranges and needn't reach their ends.
Inputs may be any that keep to these rules, and one draw needn't show every extreme that they name: `wave_order`: each zonal wavenumber 0 to 639 is held by exactly one slot. `obs_cell`: an index into the device's own block of the grid, flattened in order field, latitude, longitude; cells may repeat.
All inputs are finite; a program needn't handle non-finite values.
Results may differ from the reference program's by a relative error of at most 0.0062.
Values may be sent and summed in bfloat16 or wider, within the bound.
No kernel may reach another device: no remote copies, remote signals or barrier semaphores. Data moves between devices by JAX's collectives and lax.ppermute only.
A program may use at most 128 MiB of HBM per device.

```python
import math
import jax
import jax.numpy as jnp
from jax import lax

M = 640
NDEG = 640
NLAT = 640
NLON = 1280
OBS_DEV = 2048
F = 32
N_BAND = 8
N_LEV = 4


def with_ends(drawn, rng, least, largest):
    index_at = [jax.random.randint(jax.random.fold_in(rng, axis), (), 0, length) for axis, length in enumerate(drawn.shape)]
    widest = drawn.shape.index(max(drawn.shape))
    neighbour = index_at[:widest] + [(index_at[widest] + 1) % drawn.shape[widest]] + index_at[widest + 1:]
    return drawn.at[tuple(index_at)].set(least).at[tuple(neighbour)].set(largest)


def shard_levels(own_key, dims, shards, smallest, largest):
    loudness, own = 1.0, jax.random.fold_in(own_key, 6)
    for position, parts in shards:
        steps = jnp.exp(jax.random.uniform(jax.random.fold_in(own, position), (parts,), jnp.float32, smallest / len(shards), largest / len(shards)))
        loudness = loudness * jnp.repeat(steps, dims[position] // parts).reshape([-1 if axis == position else 1 for axis in range(len(dims))])
    return loudness


def gaussian(rng, shape, deviation, most, split=(), kind=jnp.bfloat16):
    result = jax.random.normal(rng, shape, jnp.float32) * deviation
    if len(split) > 0:
        result = shard_levels(rng, shape, split, -0.22, 0.18) * result
    return jnp.clip(result, min=-most, max=most).astype(kind)


def setup_inputs(seed: int = 0) -> dict:
    key_list = jax.random.split(jax.random.key(seed), 9)
    return {
        "spectral": gaussian(key_list[0], (2, F, M, NDEG), 0.02, 0.2, ((2, 8), (3, 4)), jnp.float32),
        "legendre": gaussian(key_list[1], (M, NDEG, NLAT), NDEG ** -0.5, 0.25, ((0, 8), (1, 4))),
        "wave_order": jax.random.permutation(key_list[2], M).astype(jnp.int32),
        "jacobian": jnp.clip(0.5 + 1.0 * jax.random.uniform(key_list[3], (F, NLAT, NLON), jnp.float32) ** shard_levels(key_list[3], (F, NLAT, NLON), ((0, 4), (1, 8)), -0.2, 0.2), 0.5, 1.5).astype(jnp.bfloat16),
        "obs_cell": with_ends(jax.random.randint(key_list[4], (N_LEV, N_BAND, OBS_DEV), 0, (F // N_LEV) * (NLAT // N_BAND) * NLON), jax.random.fold_in(key_list[4], 1), 0, ((F // N_LEV) * (NLAT // N_BAND) * NLON) - 1).astype(jnp.int32),
        "innovation": gaussian(key_list[5], (N_LEV, N_BAND, OBS_DEV), 1.0, 6.0, ((0, 4), (1, 8)), jnp.float32),
        "obs_weight": jnp.clip(jnp.exp(math.log(0.04) - 1.3862944 * jax.random.uniform(key_list[6], (N_LEV, N_BAND, OBS_DEV), jnp.float32) ** shard_levels(key_list[6], (N_LEV, N_BAND, OBS_DEV), ((0, 4), (1, 8)), -0.2, 0.2)), 0.01, 0.04),
        "inv_var": jnp.clip(jnp.exp(math.log(50.0) - 2.3025851 * jax.random.uniform(key_list[7], (NDEG,), jnp.float32) ** shard_levels(key_list[7], (NDEG,), ((0, 4),), -0.2, 0.2)), 5.0, 50.0),
    }


def fourier_table(wave_order):
    waves = wave_order.astype(jnp.int32)
    columns = jnp.arange(NLON, dtype=jnp.int32)
    phase = (waves[:, None] * columns[None, :]) % NLON
    angle = phase.astype(jnp.float32) * (2.0 * math.pi / NLON)
    factor = jnp.where(waves == 0, 1.0, 2.0).astype(jnp.float32)[:, None]
    return jnp.stack([factor * jnp.cos(angle), -factor * jnp.sin(angle)]).astype(jnp.bfloat16)


def masked_rows(legendre, wave_order, slot):
    degree = jnp.arange(NDEG, dtype=jnp.int32)
    keep = degree >= wave_order[slot]
    return jnp.where(keep[:, None], legendre[slot], jnp.zeros_like(legendre[slot]))


def reference(spectral, legendre, wave_order, jacobian, obs_cell, innovation, obs_weight, inv_var):
    spec_low = spectral.astype(jnp.bfloat16)
    slots = jnp.arange(M, dtype=jnp.int32)

    def synth(slot):
        rows = masked_rows(legendre, wave_order, slot).astype(jnp.float32)
        column = lax.dynamic_index_in_dim(spec_low, slot, 2, keepdims=False).astype(jnp.float32)
        return jnp.einsum("cfn,nl->cfl", column, rows)

    coef = jnp.moveaxis(lax.map(synth, slots), 0, 2).astype(jnp.bfloat16)
    fourier = fourier_table(wave_order)
    grid = jnp.einsum("cfsl,csj->flj", coef.astype(jnp.float32), fourier.astype(jnp.float32))
    model_grid = (grid * jacobian).astype(jnp.bfloat16)

    f_dev = F // N_LEV
    lat_dev = NLAT // N_BAND
    blocks = model_grid.reshape(N_LEV, f_dev, N_BAND, lat_dev, NLON).transpose(0, 2, 1, 3, 4)
    blocks = blocks.reshape(N_LEV, N_BAND, f_dev * lat_dev * NLON)
    picked = jnp.take_along_axis(blocks, obs_cell.astype(jnp.int32), axis=2).astype(jnp.float32)
    misfit = obs_weight * (picked - innovation)

    def spread(cells, values):
        return jnp.zeros((f_dev * lat_dev * NLON,), jnp.float32).at[cells].add(values)

    adj_blocks = jax.vmap(jax.vmap(spread))(obs_cell.astype(jnp.int32), misfit)
    grid_adj = adj_blocks.reshape(N_LEV, N_BAND, f_dev, lat_dev, NLON).transpose(0, 2, 1, 3, 4)
    grid_adj = grid_adj.reshape(F, NLAT, NLON)
    force = (grid_adj * jacobian).astype(jnp.bfloat16)
    coef_adj = jnp.einsum("csj,flj->cfsl", fourier.astype(jnp.float32), force.astype(jnp.float32)).astype(jnp.bfloat16)

    def analyse(slot):
        rows = masked_rows(legendre, wave_order, slot).astype(jnp.float32)
        column = lax.dynamic_index_in_dim(coef_adj, slot, 2, keepdims=False).astype(jnp.float32)
        return jnp.einsum("cfl,nl->cfn", column, rows)

    spec_adj = jnp.moveaxis(lax.map(analyse, slots), 0, 2)
    gradient = spectral * inv_var[None, None, None, :] + spec_adj
    return model_grid, gradient
```

```python
import functools
import math

import jax
import jax.numpy as jnp
from jax import lax
from jax.experimental import pallas as pl
from jax.experimental.pallas import tpu as pltpu
from jax.sharding import PartitionSpec as P

S_CHUNK = 16
O_CHUNK = 256
LOW = 32
SPARSE_BYTES = 48 * 2**20


def fourier_table(wave_order, width):
    columns = jnp.arange(width, dtype=jnp.int32)
    phase = wave_order[:, None] * columns[None, :] % width
    angle = phase.astype(jnp.float32) * (2.0 * math.pi / width)
    factor = jnp.where(wave_order == 0, 1.0, 2.0).astype(jnp.float32)[:, None]
    return jnp.stack([factor * jnp.cos(angle), -factor * jnp.sin(angle)]).astype(jnp.bfloat16)


def lane_tiles(width):
    return [(t, t * 128, min(width, (t + 1) * 128)) for t in range(-(-width // 128))]


def put_rows(ref, value):
    for t, lo, hi in lane_tiles(value.shape[1]):
        ref[t, :, : hi - lo] = value[:, lo:hi]


def get_rows(ref, at, width):
    pieces = [ref[t, at, :][:, : hi - lo] for t, lo, hi in lane_tiles(width)]
    return pieces[0] if len(pieces) == 1 else jnp.concatenate(pieces, axis=1)


def put_strided(ref, at, value):
    width = value.shape[1]
    for t, lo, hi in lane_tiles(width):
        piece = value[:, lo:hi]
        if hi - lo < 128:
            piece = jnp.concatenate(
                [piece, jnp.zeros((piece.shape[0], 128 - hi + lo), piece.dtype)], axis=1
            )
        ref[t, at, :] = piece


def synth_kernel(thr_ref, spec_ref, table_ref, out_ref, spec_s, coef_s, row_s):
    parts, bands = out_ref.shape[0], out_ref.shape[1]
    cf, sc, deg = spec_ref.shape
    lats = table_ref.shape[2]
    f_own = cf // 2 // parts
    l_own = lats // bands
    put_rows(spec_s, spec_ref[...].reshape(cf * sc, deg))
    degree = lax.broadcasted_iota(jnp.int32, (cf, deg), 1)
    base = pl.program_id(0) * sc
    for s in range(sc):
        a = get_rows(spec_s, pl.ds(s, cf, stride=sc), deg)
        a = jnp.where(degree >= thr_ref[base + s], a, 0.0).astype(jnp.bfloat16)
        put_strided(
            coef_s,
            pl.ds(s, cf, stride=sc),
            jnp.dot(a, table_ref[s], preferred_element_type=jnp.float32),
        )

    def regroup(i, carry):
        k = i // 2
        c = i % 2
        for f in range(f_own):
            start = pl.multiple_of(((c * parts + k) * f_own + f) * sc, sc)
            x = get_rows(coef_s, pl.ds(start, sc), lats)
            for b in range(bands):
                row_s[b, :, f * l_own : (f + 1) * l_own] = x[:, b * l_own : (b + 1) * l_own]
        for b in range(bands):
            out_ref[k, b, c, :, :] = row_s[b].astype(jnp.bfloat16)
        return carry

    lax.fori_loop(0, 2 * parts, regroup, 0)


def synth(thr, spec, table, parts, bands):
    cf, slots, deg = spec.shape
    lats = table.shape[2]
    f_own = cf // 2 // parts
    l_own = lats // bands
    sc = S_CHUNK
    return pl.pallas_call(
        synth_kernel,
        grid_spec=pltpu.PrefetchScalarGridSpec(
            num_scalar_prefetch=1,
            grid=(slots // sc,),
            in_specs=[
                pl.BlockSpec((cf, sc, deg), lambda i, t: (0, i, 0)),
                pl.BlockSpec((sc, deg, lats), lambda i, t: (i, 0, 0)),
            ],
            out_specs=pl.BlockSpec(
                (parts, bands, 2, sc, f_own * l_own), lambda i, t: (0, 0, 0, i, 0)
            ),
            scratch_shapes=[
                pltpu.VMEM((-(-deg // 128), cf * sc, 128), jnp.float32),
                pltpu.VMEM((-(-lats // 128), cf * sc, 128), jnp.float32),
                pltpu.VMEM((bands, sc, f_own * l_own), jnp.float32),
            ],
        ),
        out_shape=jax.ShapeDtypeStruct((parts, bands, 2, slots, f_own * l_own), jnp.bfloat16),
        compiler_params=pltpu.CompilerParams(
            dimension_semantics=("arbitrary",), vmem_limit_bytes=40 * 2**20
        ),
        name="synth",
    )(thr, spec, table)


def pick_kernel(coef_ref, row_ref, high_ref, low_ref, tab_ref, g_ref, p_ref):
    cs, rows = coef_ref.shape[1], coef_ref.shape[2]
    slots = cs // 2
    obs = row_ref.shape[2]
    highs = (tab_ref.shape[1] - 2 * LOW) // 2
    row_id = lax.broadcasted_iota(jnp.int32, (rows, O_CHUNK), 0)
    high_id = lax.broadcasted_iota(jnp.int32, (highs, O_CHUNK), 0)
    low_id = lax.broadcasted_iota(jnp.int32, (LOW, O_CHUNK), 0)
    for o in range(obs // O_CHUNK):
        at = slice(o * O_CHUNK, (o + 1) * O_CHUNK)
        a = (high_id == high_ref[0, :, at]).astype(jnp.float32)
        b = (low_id == low_ref[0, :, at]).astype(jnp.float32)
        hot = jnp.concatenate([a, a, b, b], axis=0).astype(jnp.bfloat16)
        parts = jnp.dot(tab_ref[...], hot, preferred_element_type=jnp.float32)
        uc, us = parts[:slots], parts[slots : 2 * slots]
        vc, vs = parts[2 * slots : 3 * slots], parts[3 * slots :]
        gc = (uc * vc - us * vs).astype(jnp.bfloat16)
        gs = (-(us * vc + uc * vs)).astype(jnp.bfloat16)
        g_ref[0, :slots, at] = gc
        g_ref[0, slots:, at] = gs
        pick = (row_id == row_ref[0, :, at]).astype(jnp.float32).astype(jnp.bfloat16)
        t = jnp.dot(coef_ref[0], pick, preferred_element_type=jnp.float32)
        p = t[:slots] * gc.astype(jnp.float32) + t[slots:] * gs.astype(jnp.float32)
        p_ref[0, :, at] = jnp.sum(p, axis=0, keepdims=True)


def pick(coef, row, high, low, tab):
    blocks, cs, rows = coef.shape
    obs = row.shape[2]
    one = pl.BlockSpec((1, 1, obs), lambda i: (i, 0, 0))
    return pl.pallas_call(
        pick_kernel,
        grid=(blocks,),
        in_specs=[
            pl.BlockSpec((1, cs, rows), lambda i: (i, 0, 0)),
            one,
            one,
            one,
            pl.BlockSpec(tab.shape, lambda i: (0, 0)),
        ],
        out_specs=[pl.BlockSpec((1, cs, obs), lambda i: (i, 0, 0)), one],
        out_shape=[
            jax.ShapeDtypeStruct((blocks, cs, obs), jnp.bfloat16),
            jax.ShapeDtypeStruct((blocks, 1, obs), jnp.float32),
        ],
        compiler_params=pltpu.CompilerParams(
            dimension_semantics=("arbitrary",), vmem_limit_bytes=40 * 2**20
        ),
        name="pick",
    )(coef, row, high, low, tab)


def spread_kernel(g_ref, row_ref, val_ref, out_ref, hot_s, coef_s, *, bands):
    cs, obs = g_ref.shape[1], g_ref.shape[2]
    slots = cs // 2
    f_own = out_ref.shape[1]
    lats = out_ref.shape[3]
    l_own = lats // bands
    rows = f_own * l_own
    row_id = lax.broadcasted_iota(jnp.int32, (rows, O_CHUNK), 0)
    for o in range(obs // O_CHUNK):
        at = slice(o * O_CHUNK, (o + 1) * O_CHUNK)
        hot_s[:, at] = jnp.where(row_id == row_ref[0, :, at], val_ref[0, :, at], 0.0).astype(
            jnp.bfloat16
        )
    acc = lax.dot_general(
        hot_s[...], g_ref[0], (((1,), (1,)), ((), ())), preferred_element_type=jnp.float32
    )
    b = pl.program_id(1)
    start = pl.multiple_of(b * l_own, 8)
    for f in range(f_own):
        coef_s[f, pl.ds(start, l_own), :] = acc[f * l_own : (f + 1) * l_own]

    @pl.when(b == bands - 1)
    def _():
        for f in range(f_own):
            t = coef_s[f].T.astype(jnp.bfloat16)
            out_ref[0, f] = t[:slots]
            out_ref[1, f] = t[slots:]


def spread(g, row, val, parts, bands, fields, lats):
    blocks, cs, obs = g.shape
    f_own = fields // parts
    l_own = lats // bands
    one = pl.BlockSpec((1, 1, obs), lambda k, b: (k * bands + b, 0, 0))
    return pl.pallas_call(
        functools.partial(spread_kernel, bands=bands),
        grid=(parts, bands),
        in_specs=[pl.BlockSpec((1, cs, obs), lambda k, b: (k * bands + b, 0, 0)), one, one],
        out_specs=pl.BlockSpec((2, f_own, cs // 2, lats), lambda k, b: (0, k, 0, 0)),
        out_shape=jax.ShapeDtypeStruct((2, fields, cs // 2, lats), jnp.bfloat16),
        scratch_shapes=[
            pltpu.VMEM((f_own * l_own, obs), jnp.bfloat16),
            pltpu.VMEM((f_own, lats, cs), jnp.float32),
        ],
        compiler_params=pltpu.CompilerParams(
            dimension_semantics=("arbitrary", "arbitrary"), vmem_limit_bytes=40 * 2**20
        ),
        name="spread",
    )(g, row, val)


def analyse_kernel(thr_ref, coef_ref, table_ref, spec_ref, inv_ref, out_ref, coef_s, out_s):
    cf, sc, lats = coef_ref.shape
    deg = spec_ref.shape[2]
    put_rows(coef_s, coef_ref[...].astype(jnp.float32).reshape(cf * sc, lats))
    degree = lax.broadcasted_iota(jnp.int32, (cf, deg), 1)
    base = pl.program_id(0) * sc
    for s in range(sc):
        a = get_rows(coef_s, pl.ds(s, cf, stride=sc), lats).astype(jnp.bfloat16)
        o = lax.dot_general(
            a, table_ref[s], (((1,), (1,)), ((), ())), preferred_element_type=jnp.float32
        )
        put_strided(
            out_s, pl.ds(s, cf, stride=sc), jnp.where(degree >= thr_ref[base + s], o, 0.0)
        )
    adj = get_rows(out_s, slice(None), deg).reshape(cf, sc, deg)
    out_ref[...] = spec_ref[...] * inv_ref[...][None] + adj


def analyse(thr, coef, table, spec, inv_var):
    cf, slots, lats = coef.shape
    deg = spec.shape[2]
    sc = S_CHUNK
    return pl.pallas_call(
        analyse_kernel,
        grid_spec=pltpu.PrefetchScalarGridSpec(
            num_scalar_prefetch=1,
            grid=(slots // sc,),
            in_specs=[
                pl.BlockSpec((cf, sc, lats), lambda i, t: (0, i, 0)),
                pl.BlockSpec((sc, deg, lats), lambda i, t: (i, 0, 0)),
                pl.BlockSpec((cf, sc, deg), lambda i, t: (0, i, 0)),
                pl.BlockSpec((1, deg), lambda i, t: (0, 0)),
            ],
            out_specs=pl.BlockSpec((cf, sc, deg), lambda i, t: (0, i, 0)),
            scratch_shapes=[
                pltpu.VMEM((-(-lats // 128), cf * sc, 128), jnp.float32),
                pltpu.VMEM((-(-deg // 128), cf * sc, 128), jnp.float32),
            ],
        ),
        out_shape=jax.ShapeDtypeStruct((cf, slots, deg), jnp.float32),
        compiler_params=pltpu.CompilerParams(
            dimension_semantics=("arbitrary",), vmem_limit_bytes=40 * 2**20
        ),
        name="analyse",
    )(thr, coef, table, spec, inv_var)


def observation_table(waves, width):
    highs = width // LOW
    factor = jnp.where(waves == 0, 1.0, 2.0).astype(jnp.float32)[:, None]

    def pair(columns, scale):
        phase = waves[:, None] * columns[None, :] % width
        angle = phase.astype(jnp.float32) * (2.0 * math.pi / width)
        exact = jnp.concatenate([scale * jnp.cos(angle), scale * jnp.sin(angle)], axis=0)
        near = exact.astype(jnp.bfloat16)
        rest = (exact - near.astype(jnp.float32)).astype(jnp.bfloat16)
        return jnp.concatenate([near, rest], axis=1)

    u = pair(LOW * jnp.arange(highs, dtype=jnp.int32), factor)
    v = pair(jnp.arange(LOW, dtype=jnp.int32), 1.0)
    top = jnp.concatenate([u, jnp.zeros((u.shape[0], v.shape[1]), u.dtype)], axis=1)
    bottom = jnp.concatenate([jnp.zeros((v.shape[0], u.shape[1]), u.dtype), v], axis=1)
    return jnp.concatenate([top, bottom], axis=0)


def sparse_shards(parts, bands, spectral, legendre, wave_order, jacobian, obs_cell, innovation, obs_weight, inv_var):
    _, fields, slots, degrees = spectral.shape
    lats = legendre.shape[2]
    f_own, l_own, width = jacobian.shape
    obs = obs_cell.shape[-1]
    own_waves = lax.dynamic_slice_in_dim(wave_order, lax.axis_index("band") * slots, slots)
    thr = own_waves - lax.axis_index("lev") * degrees
    spec = spectral.reshape(2 * fields, slots, degrees)

    partial = synth(thr, spec, legendre, parts, bands)
    summed = lax.psum_scatter(
        partial.reshape(parts, bands * 2 * slots, f_own * l_own), "lev", scatter_dimension=0, tiled=True
    )

    cells = obs_cell.reshape(1, 1, obs)
    all_cells = lax.all_gather(cells, ("lev", "band"), axis=0, tiled=True)
    row = all_cells // width
    lon = all_cells % width
    g, p = pick(
        partial.reshape(parts * bands, 2 * slots, f_own * l_own),
        row,
        lon // LOW,
        lon % LOW,
        observation_table(own_waves, width),
    )
    at_owner = lax.all_to_all(p, ("lev", "band"), split_axis=0, concat_axis=0, tiled=True)
    grid_at = jnp.sum(at_owner.reshape(parts * bands, obs), axis=0)
    jac_at = jacobian.reshape(-1)[obs_cell.reshape(-1)].astype(jnp.float32)
    misfit = obs_weight.reshape(-1) * (grid_at * jac_at - innovation.reshape(-1))
    val = lax.all_gather((misfit * jac_at).reshape(1, 1, obs), ("lev", "band"), axis=0, tiled=True)
    coef_adj = spread(g, row, val, parts, bands, fields, lats)
    gradient = analyse(
        thr,
        coef_adj.reshape(2 * fields, slots, lats),
        legendre,
        spec,
        inv_var.reshape(1, degrees),
    ).reshape(spectral.shape)

    by_latitude = lax.all_to_all(
        summed.reshape(bands, 2 * slots, f_own * l_own), "band", split_axis=0, concat_axis=0, tiled=True
    )
    fourier = fourier_table(wave_order, width).reshape(2, bands, slots, width)
    fourier = fourier.transpose(1, 0, 2, 3).reshape(bands * 2 * slots, width)
    grid = lax.dot_general(
        by_latitude.reshape(bands * 2 * slots, f_own * l_own),
        fourier,
        (((0,), (0,)), ((), ())),
        preferred_element_type=jnp.float32,
    )
    model_grid = (grid * jacobian.reshape(f_own * l_own, width)).astype(jnp.bfloat16)
    return model_grid.reshape(jacobian.shape), gradient


def dense_shards(spectral, legendre, wave_order, jacobian, obs_cell, innovation, obs_weight, inv_var):
    slot_count = spectral.shape[2]
    degree_count = spectral.shape[3]
    own_waves = lax.dynamic_slice_in_dim(
        wave_order, lax.axis_index("band") * slot_count, slot_count
    )
    degree = lax.axis_index("lev") * degree_count + jnp.arange(degree_count, dtype=jnp.int32)
    keep = degree[None, :, None] >= own_waves[:, None, None]
    table = jnp.where(keep, legendre, jnp.zeros_like(legendre))
    spec_low = spectral.astype(jnp.bfloat16)
    fourier = fourier_table(wave_order, jacobian.shape[2])
    summed = lax.psum_scatter(
        jnp.einsum("cfsn,snl->fcsl", spec_low, table, preferred_element_type=jnp.float32),
        "lev",
        scatter_dimension=0,
        tiled=True,
    )
    by_latitude = lax.all_to_all(
        summed.astype(jnp.bfloat16), "band", split_axis=3, concat_axis=2, tiled=True
    )
    grid = lax.dot_general(
        by_latitude, fourier, (((1, 2), (0, 1)), ((), ())), preferred_element_type=jnp.float32
    )
    model_grid = (grid * jacobian).astype(jnp.bfloat16)
    cells = obs_cell.reshape(-1)
    picked = model_grid.reshape(-1)[cells].astype(jnp.float32)
    misfit = obs_weight.reshape(-1) * (picked - innovation.reshape(-1))
    grid_adj = (
        jnp.zeros((model_grid.size,), jnp.float32).at[cells].add(misfit).reshape(model_grid.shape)
    )
    force = (grid_adj * jacobian).astype(jnp.bfloat16)
    coef_adj = jnp.einsum(
        "csj,flj->fcsl", fourier, force, preferred_element_type=jnp.float32
    ).astype(jnp.bfloat16)
    by_wave = lax.all_to_all(coef_adj, "band", split_axis=2, concat_axis=3, tiled=True)
    spec_adj = jnp.einsum(
        "fcsl,snl->cfsn",
        lax.all_gather(by_wave, "lev", axis=0, tiled=True),
        table,
        preferred_element_type=jnp.float32,
    )
    gradient = spectral * inv_var[None, None, None, :] + spec_adj
    return (model_grid, gradient)


def solution(mesh):
    parts, bands = mesh.shape["lev"], mesh.shape["band"]

    def shards(spectral, legendre, wave_order, jacobian, obs_cell, innovation, obs_weight, inv_var):
        slots = spectral.shape[2]
        l_own, width = jacobian.shape[1:]
        obs = obs_cell.shape[-1]
        table_bytes = parts * bands * obs * 4 * slots
        fits = (
            table_bytes <= SPARSE_BYTES
            and slots % S_CHUNK == 0
            and l_own % 16 == 0
            and obs % O_CHUNK == 0
            and width % LOW == 0
        )
        args = (spectral, legendre, wave_order, jacobian, obs_cell, innovation, obs_weight, inv_var)
        return sparse_shards(parts, bands, *args) if fits else dense_shards(*args)

    in_specs = (
        P(None, None, "band", "lev"),
        P("band", "lev", None),
        P(),
        P("lev", "band", None),
        P("lev", "band", None),
        P("lev", "band", None),
        P("lev", "band", None),
        P("lev"),
    )
    out_specs = (P("lev", "band", None), P(None, None, "band", "lev"))
    return jax.shard_map(shards, mesh=mesh, in_specs=in_specs, out_specs=out_specs, check_vma=False)
```

```python
import functools
import math

import jax
import jax.numpy as jnp
from jax import lax
from jax.experimental import pallas as pl
from jax.experimental.pallas import tpu as pltpu
from jax.sharding import PartitionSpec as P

S_CHUNK = 16
SPREAD_CHUNK = 512
O_CHUNK = 256
VMEM_BYTES = 60 * 2**20
HIGH_ROOM = 1024
LOW = 32
SPARSE_BYTES = 48 * 2**20


def fourier_table(wave_order, width):
    columns = jnp.arange(width, dtype=jnp.int32)
    phase = wave_order[:, None] * columns[None, :] % width
    angle = phase.astype(jnp.float32) * (2.0 * math.pi / width)
    factor = jnp.where(wave_order == 0, 1.0, 2.0).astype(jnp.float32)[:, None]
    return jnp.stack([factor * jnp.cos(angle), -factor * jnp.sin(angle)]).astype(jnp.bfloat16)


def lane_tiles(width):
    return [(t, t * 128, min(width, (t + 1) * 128)) for t in range(-(-width // 128))]


def put_rows(ref, value):
    for t, lo, hi in lane_tiles(value.shape[1]):
        ref[t, :, : hi - lo] = value[:, lo:hi]


def get_rows(ref, at, width):
    pieces = [ref[t, at, :][:, : hi - lo] for t, lo, hi in lane_tiles(width)]
    return pieces[0] if len(pieces) == 1 else jnp.concatenate(pieces, axis=1)


def put_strided(ref, at, value):
    width = value.shape[1]
    for t, lo, hi in lane_tiles(width):
        piece = value[:, lo:hi]
        if hi - lo < 128:
            piece = jnp.concatenate(
                [piece, jnp.zeros((piece.shape[0], 128 - hi + lo), piece.dtype)], axis=1
            )
        ref[t, at, :] = piece


def synth_kernel(thr_ref, spec_ref, table_ref, out_ref, spec_s, coef_s, *, first):
    parts, bands = out_ref.shape[0], out_ref.shape[1]
    cf, sc, deg = spec_ref.shape
    lats = table_ref.shape[2]
    f_own = cf // 2 // parts
    l_own = lats // bands
    put_rows(spec_s, spec_ref[...].reshape(cf * sc, deg))
    degree = lax.broadcasted_iota(jnp.int32, (cf, deg), 1)
    base = (first + pl.program_id(0)) * sc
    for s in range(sc):
        a = get_rows(spec_s, pl.ds(s, cf, stride=sc), deg)
        a = jnp.where(degree >= thr_ref[base + s], a, 0.0).astype(jnp.bfloat16)
        put_strided(
            coef_s,
            pl.ds(s, cf, stride=sc),
            jnp.dot(a, table_ref[s], preferred_element_type=jnp.float32),
        )

    def regroup(i, carry):
        k = i // 2
        c = i % 2
        x = []
        for f in range(f_own):
            start = pl.multiple_of(((c * parts + k) * f_own + f) * sc, sc)
            x.append(get_rows(coef_s, pl.ds(start, sc), lats).astype(jnp.bfloat16))
        for b in range(bands):
            out_ref[k, b, c, :, :] = jnp.concatenate(
                [x[f][:, b * l_own : (b + 1) * l_own] for f in range(f_own)], axis=1
            )
        return carry

    lax.fori_loop(0, 2 * parts, regroup, 0)


def synth(thr, spec, table, parts, bands, first, count):
    cf, _, deg = spec.shape
    lats = table.shape[2]
    f_own = cf // 2 // parts
    l_own = lats // bands
    sc = S_CHUNK
    return pl.pallas_call(
        functools.partial(synth_kernel, first=first),
        grid_spec=pltpu.PrefetchScalarGridSpec(
            num_scalar_prefetch=1,
            grid=(count,),
            in_specs=[
                pl.BlockSpec((cf, sc, deg), lambda i, t: (0, first + i, 0)),
                pl.BlockSpec((sc, deg, lats), lambda i, t: (first + i, 0, 0)),
            ],
            out_specs=pl.BlockSpec(
                (parts, bands, 2, sc, f_own * l_own), lambda i, t: (0, 0, 0, i, 0)
            ),
            scratch_shapes=[
                pltpu.VMEM((-(-deg // 128), cf * sc, 128), jnp.float32),
                pltpu.VMEM((-(-lats // 128), cf * sc, 128), jnp.float32),
            ],
        ),
        out_shape=jax.ShapeDtypeStruct((parts, bands, 2, count * sc, f_own * l_own), jnp.bfloat16),
        compiler_params=pltpu.CompilerParams(
            dimension_semantics=("arbitrary",), vmem_limit_bytes=VMEM_BYTES
        ),
        name="synth",
    )(thr, spec, table)


def one_hot(cells, rows, values=None):
    row = (cells // (LOW * HIGH_ROOM)).astype(jnp.int16)
    row_id = lax.broadcasted_iota(jnp.int16, (rows, cells.shape[1]), 0)
    values = jnp.ones(cells.shape, jnp.bfloat16) if values is None else values.astype(jnp.bfloat16)
    return jnp.where(row_id == row, values, jnp.zeros_like(values))


def pick_kernel(cell_ref, tab_ref, *refs):
    coef_refs, (g_ref, p_ref) = refs[:-2], refs[-2:]
    coef = jnp.concatenate([r[0] for r in coef_refs], axis=0)
    rows = coef.shape[1]
    slots = coef.shape[0] // 2
    obs = cell_ref.shape[2]
    for o in range(obs // O_CHUNK):
        at = slice(o * O_CHUNK, (o + 1) * O_CHUNK)
        t = jnp.dot(coef, one_hot(cell_ref[0, :, at], rows), preferred_element_type=jnp.float32)
        for lane in range(0, O_CHUNK, 128):
            own_at = slice(o * O_CHUNK + lane, o * O_CHUNK + lane + 128)
            cell = cell_ref[0, :, own_at]
            high = jnp.broadcast_to((cell // LOW) & (HIGH_ROOM - 1), (slots, 128))
            low = jnp.broadcast_to(cell & (LOW - 1), (slots, 128))

            def look_up(i, index):
                return jnp.take_along_axis(tab_ref[i], index, axis=1, mode="promise_in_bounds")

            uc, us = look_up(0, high), look_up(1, high)
            vc, vs = look_up(2, low), look_up(3, low)
            gc = (uc * vc - us * vs).astype(jnp.bfloat16)
            gs = (-(us * vc + uc * vs)).astype(jnp.bfloat16)
            g_ref[0, :slots, own_at] = gc
            g_ref[0, slots:, own_at] = gs
            order, first = [], 0
            for r in coef_refs:
                own = slice(first, first + r.shape[1] // 2)
                order += [gc[own], gs[own]]
                first = own.stop
            p = t[:, lane : lane + 128] * jnp.concatenate(order, axis=0).astype(jnp.float32)
            p_ref[0, :, own_at] = jnp.sum(p, axis=0, keepdims=True)


def pick(coefs, cells, tab):
    blocks, _, rows = coefs[0].shape
    cs = sum(x.shape[1] for x in coefs)
    obs = cells.shape[2]
    one = pl.BlockSpec((1, 1, obs), lambda i: (i, 0, 0))
    return pl.pallas_call(
        pick_kernel,
        grid=(blocks,),
        in_specs=[one, pl.BlockSpec(tab.shape, lambda i: (0, 0, 0))]
        + [pl.BlockSpec((1, x.shape[1], rows), lambda i: (i, 0, 0)) for x in coefs],
        out_specs=[pl.BlockSpec((1, cs, obs), lambda i: (i, 0, 0)), one],
        out_shape=[
            jax.ShapeDtypeStruct((blocks, cs, obs), jnp.bfloat16),
            jax.ShapeDtypeStruct((blocks, 1, obs), jnp.float32),
        ],
        compiler_params=pltpu.CompilerParams(
            dimension_semantics=("arbitrary",), vmem_limit_bytes=VMEM_BYTES
        ),
        name="pick",
    )(cells, tab, *coefs)


def spread_kernel(g_ref, cell_ref, val_ref, out_ref, coef_s, *, bands):
    cs, obs = g_ref.shape[1], g_ref.shape[2]
    slots = cs // 2
    f_own = out_ref.shape[1]
    lats = out_ref.shape[3]
    l_own = lats // bands
    rows = f_own * l_own
    acc = 0.0
    for o in range(obs // SPREAD_CHUNK):
        at = slice(o * SPREAD_CHUNK, (o + 1) * SPREAD_CHUNK)
        acc = acc + lax.dot_general(
            one_hot(cell_ref[0, :, at], rows, val_ref[0, :, at]),
            g_ref[0, :, at],
            (((1,), (1,)), ((), ())),
            preferred_element_type=jnp.float32,
        )
    b = pl.program_id(1)
    start = pl.multiple_of(b * l_own, 8)
    for f in range(f_own):
        coef_s[f, pl.ds(start, l_own), :] = acc[f * l_own : (f + 1) * l_own]

    @pl.when(b == bands - 1)
    def _():
        for f in range(f_own):
            t = coef_s[f].T.astype(jnp.bfloat16)
            out_ref[0, f] = t[:slots]
            out_ref[1, f] = t[slots:]


def spread(g, cells, val, parts, bands, fields, lats):
    _, cs, obs = g.shape
    f_own = fields // parts
    one = pl.BlockSpec((1, 1, obs), lambda k, b: (k * bands + b, 0, 0))
    return pl.pallas_call(
        functools.partial(spread_kernel, bands=bands),
        grid=(parts, bands),
        in_specs=[pl.BlockSpec((1, cs, obs), lambda k, b: (k * bands + b, 0, 0)), one, one],
        out_specs=pl.BlockSpec((2, f_own, cs // 2, lats), lambda k, b: (0, k, 0, 0)),
        out_shape=jax.ShapeDtypeStruct((2, fields, cs // 2, lats), jnp.bfloat16),
        scratch_shapes=[
            pltpu.VMEM((f_own, lats, cs), jnp.float32),
        ],
        compiler_params=pltpu.CompilerParams(
            dimension_semantics=("arbitrary", "arbitrary"), vmem_limit_bytes=VMEM_BYTES
        ),
        name="spread",
    )(g, cells, val)


def fourier_kernel(base_ref, step_ref, out_ref):
    bc, bs = base_ref[0], base_ref[1]
    for t in range(out_ref.shape[3] // 128):
        at = slice(t * 128, (t + 1) * 128)
        sc, ss = step_ref[0, :, t : t + 1], step_ref[1, :, t : t + 1]
        out_ref[0, 0, :, at] = (sc * bc - ss * bs).astype(jnp.bfloat16)
        out_ref[0, 1, :, at] = (-(ss * bc + sc * bs)).astype(jnp.bfloat16)


def fourier_rows(wave_order, width, slots):
    count = wave_order.shape[0]
    factor = jnp.where(wave_order == 0, 1.0, 2.0).astype(jnp.float32)[:, None]

    def pair(columns, scale):
        phase = wave_order[:, None] * columns[None, :] % width
        angle = phase.astype(jnp.float32) * (2.0 * math.pi / width)
        return jnp.stack([scale * jnp.cos(angle), scale * jnp.sin(angle)])

    base = pair(jnp.arange(128, dtype=jnp.int32), 1.0)
    step = pair(128 * jnp.arange(width // 128, dtype=jnp.int32), factor)
    rows = pl.pallas_call(
        fourier_kernel,
        grid=(count // slots,),
        in_specs=[
            pl.BlockSpec((2, slots, 128), lambda i: (0, i, 0)),
            pl.BlockSpec((2, slots, width // 128), lambda i: (0, i, 0)),
        ],
        out_specs=pl.BlockSpec((1, 2, slots, width), lambda i: (i, 0, 0, 0)),
        out_shape=jax.ShapeDtypeStruct((count // slots, 2, slots, width), jnp.bfloat16),
        compiler_params=pltpu.CompilerParams(
            dimension_semantics=("arbitrary",), vmem_limit_bytes=VMEM_BYTES
        ),
        name="fourier",
    )(base, step)
    return rows


def analyse_kernel(thr_ref, coef_ref, table_ref, spec_ref, inv_ref, out_ref, coef_s, out_s):
    cf, sc, lats = coef_ref.shape
    deg = spec_ref.shape[2]
    put_rows(coef_s, coef_ref[...].astype(jnp.float32).reshape(cf * sc, lats))
    degree = lax.broadcasted_iota(jnp.int32, (cf, deg), 1)
    base = pl.program_id(0) * sc
    for s in range(sc):
        a = get_rows(coef_s, pl.ds(s, cf, stride=sc), lats).astype(jnp.bfloat16)
        o = lax.dot_general(
            a, table_ref[s], (((1,), (1,)), ((), ())), preferred_element_type=jnp.float32
        )
        put_strided(
            out_s, pl.ds(s, cf, stride=sc), jnp.where(degree >= thr_ref[base + s], o, 0.0)
        )
    adj = get_rows(out_s, slice(None), deg).reshape(cf, sc, deg)
    out_ref[...] = spec_ref[...] * inv_ref[...][None] + adj


def analyse(thr, coef, table, spec, inv_var):
    cf, slots, lats = coef.shape
    deg = spec.shape[2]
    sc = S_CHUNK
    return pl.pallas_call(
        analyse_kernel,
        grid_spec=pltpu.PrefetchScalarGridSpec(
            num_scalar_prefetch=1,
            grid=(slots // sc,),
            in_specs=[
                pl.BlockSpec((cf, sc, lats), lambda i, t: (0, i, 0)),
                pl.BlockSpec((sc, deg, lats), lambda i, t: (i, 0, 0)),
                pl.BlockSpec((cf, sc, deg), lambda i, t: (0, i, 0)),
                pl.BlockSpec((1, deg), lambda i, t: (0, 0)),
            ],
            out_specs=pl.BlockSpec((cf, sc, deg), lambda i, t: (0, i, 0)),
            scratch_shapes=[
                pltpu.VMEM((-(-lats // 128), cf * sc, 128), jnp.float32),
                pltpu.VMEM((-(-deg // 128), cf * sc, 128), jnp.float32),
            ],
        ),
        out_shape=jax.ShapeDtypeStruct((cf, slots, deg), jnp.float32),
        compiler_params=pltpu.CompilerParams(
            dimension_semantics=("arbitrary",), vmem_limit_bytes=VMEM_BYTES
        ),
        name="analyse",
    )(thr, coef, table, spec, inv_var)


def observation_table(waves, width):
    factor = jnp.where(waves == 0, 1.0, 2.0).astype(jnp.float32)[:, None]
    columns = jnp.arange(128, dtype=jnp.int32)

    def pair(step, scale):
        angle = (waves[:, None] * (step * columns)[None, :] % width).astype(jnp.float32)
        angle = angle * (2.0 * math.pi / width)
        return [scale * jnp.cos(angle), scale * jnp.sin(angle)]

    return jnp.stack(pair(LOW, factor) + pair(1, 1.0))


def chunk_counts(steps):
    return [steps] if steps < 2 else [steps - steps * 2 // 5, steps * 2 // 5]


def sparse_shards(parts, bands, spectral, legendre, wave_order, jacobian, obs_cell, innovation, obs_weight, inv_var):
    _, fields, slots, degrees = spectral.shape
    lats = legendre.shape[2]
    f_own, l_own, width = jacobian.shape
    obs = obs_cell.shape[-1]
    own_waves = lax.dynamic_slice_in_dim(wave_order, lax.axis_index("band") * slots, slots)
    thr = own_waves - lax.axis_index("lev") * degrees
    spec = spectral.reshape(2 * fields, slots, degrees)

    def to_all(x):
        copies = jnp.broadcast_to(x.reshape(1, 1, obs), (parts * bands, 1, obs))
        return lax.all_to_all(copies, ("lev", "band"), split_axis=0, concat_axis=0, tiled=True)

    lon = obs_cell % width
    cells = to_all((obs_cell // width) * (HIGH_ROOM * LOW) + lon)
    counts = chunk_counts(slots // S_CHUNK)
    partial, summed, first = [], [], 0
    for count in counts:
        x = synth(thr, spec, legendre, parts, bands, first, count)
        first += count
        x = x.reshape(parts, bands * 2 * count * S_CHUNK, f_own * l_own)
        partial.append(x)
        summed.append(lax.psum_scatter(x, "lev", scatter_dimension=0, tiled=True))

    g, p = pick(
        [x.reshape(parts * bands, -1, f_own * l_own) for x in partial],
        cells,
        observation_table(own_waves, width),
    )
    at_owner = lax.all_to_all(p, ("lev", "band"), split_axis=0, concat_axis=0, tiled=True)
    jac_at = jacobian.reshape(-1)[obs_cell.reshape(-1)].astype(jnp.float32)
    grid_at = jnp.sum(at_owner.reshape(parts * bands, obs), axis=0)
    misfit = obs_weight.reshape(-1) * (grid_at * jac_at - innovation.reshape(-1))
    val = to_all(misfit * jac_at)
    fourier = fourier_rows(wave_order, width, slots)
    val, early, fourier = lax.optimization_barrier((val, summed[:-1], fourier))
    coef_adj = spread(g, cells, val, parts, bands, fields, lats)
    coef_adj, late = lax.optimization_barrier((coef_adj, summed[-1]))
    gradient = analyse(
        thr,
        coef_adj.reshape(2 * fields, slots, lats),
        legendre,
        spec,
        inv_var.reshape(1, degrees),
    ).reshape(spectral.shape)

    grid, first = 0.0, 0
    for count, x in zip(counts, [*early, late]):
        n = count * S_CHUNK
        x = lax.all_to_all(
            x.reshape(bands, 2 * n, f_own * l_own), "band", split_axis=0, concat_axis=0, tiled=True
        )
        grid = grid + lax.dot_general(
            x.reshape(bands, 2, n, f_own * l_own),
            fourier[:, :, first : first + n],
            (((0, 1, 2), (0, 1, 2)), ((), ())),
            preferred_element_type=jnp.float32,
        )
        first += n
    model_grid = (grid * jacobian.reshape(f_own * l_own, width)).astype(jnp.bfloat16)
    return model_grid.reshape(jacobian.shape), gradient


def dense_shards(spectral, legendre, wave_order, jacobian, obs_cell, innovation, obs_weight, inv_var):
    slot_count = spectral.shape[2]
    degree_count = spectral.shape[3]
    own_waves = lax.dynamic_slice_in_dim(
        wave_order, lax.axis_index("band") * slot_count, slot_count
    )
    degree = lax.axis_index("lev") * degree_count + jnp.arange(degree_count, dtype=jnp.int32)
    keep = degree[None, :, None] >= own_waves[:, None, None]
    table = jnp.where(keep, legendre, jnp.zeros_like(legendre))
    spec_low = spectral.astype(jnp.bfloat16)
    fourier = fourier_table(wave_order, jacobian.shape[2])
    summed = lax.psum_scatter(
        jnp.einsum("cfsn,snl->fcsl", spec_low, table, preferred_element_type=jnp.float32),
        "lev",
        scatter_dimension=0,
        tiled=True,
    )
    by_latitude = lax.all_to_all(
        summed.astype(jnp.bfloat16), "band", split_axis=3, concat_axis=2, tiled=True
    )
    grid = lax.dot_general(
        by_latitude, fourier, (((1, 2), (0, 1)), ((), ())), preferred_element_type=jnp.float32
    )
    model_grid = (grid * jacobian).astype(jnp.bfloat16)
    cells = obs_cell.reshape(-1)
    picked = model_grid.reshape(-1)[cells].astype(jnp.float32)
    misfit = obs_weight.reshape(-1) * (picked - innovation.reshape(-1))
    grid_adj = (
        jnp.zeros((model_grid.size,), jnp.float32).at[cells].add(misfit).reshape(model_grid.shape)
    )
    force = (grid_adj * jacobian).astype(jnp.bfloat16)
    coef_adj = jnp.einsum(
        "csj,flj->fcsl", fourier, force, preferred_element_type=jnp.float32
    ).astype(jnp.bfloat16)
    by_wave = lax.all_to_all(coef_adj, "band", split_axis=2, concat_axis=3, tiled=True)
    spec_adj = jnp.einsum(
        "fcsl,snl->cfsn",
        lax.all_gather(by_wave, "lev", axis=0, tiled=True),
        table,
        preferred_element_type=jnp.float32,
    )
    gradient = spectral * inv_var[None, None, None, :] + spec_adj
    return (model_grid, gradient)


def solution(mesh):
    parts, bands = mesh.shape["lev"], mesh.shape["band"]

    def shards(spectral, legendre, wave_order, jacobian, obs_cell, innovation, obs_weight, inv_var):
        slots = spectral.shape[2]
        l_own, width = jacobian.shape[1:]
        obs = obs_cell.shape[-1]
        table_bytes = parts * bands * obs * 4 * slots
        fits = (
            table_bytes <= SPARSE_BYTES
            and slots % S_CHUNK == 0
            and l_own % 16 == 0
            and obs % O_CHUNK == 0
            and obs % SPREAD_CHUNK == 0
            and width // LOW <= 128
            and width % LOW == 0
            and width % 128 == 0
        )
        args = (spectral, legendre, wave_order, jacobian, obs_cell, innovation, obs_weight, inv_var)
        return sparse_shards(parts, bands, *args) if fits else dense_shards(*args)

    in_specs = (
        P(None, None, "band", "lev"),
        P("band", "lev", None),
        P(),
        P("lev", "band", None),
        P("lev", "band", None),
        P("lev", "band", None),
        P("lev", "band", None),
        P("lev"),
    )
    out_specs = (P("lev", "band", None), P(None, None, "band", "lev"))
    return jax.shard_map(shards, mesh=mesh, in_specs=in_specs, out_specs=out_specs, check_vma=False)
```
